32 devices in a mesh: gx: 4 (over x, core), gy: 4 (over z), gz: 2 (over y).
Axes of the slice: x: 2, y: 2, z: 4, core: 2. Of those that a mesh axis runs over, the one named last changes fastest.
Arguments:
- traces: bfloat16 [2, 4, 4, 2, 512, 768], P(None, 'gx', 'gy', 'gz'), may hold values from -6 to 6
- sources: bfloat16 [2, 4, 4, 2, 512, 768], P(None, 'gx', 'gy', 'gz'), may hold values from -4 to 4
- local_ops: bfloat16 [2, 4, 4, 2, 768, 768], P(None, 'gx', 'gy', 'gz'), may hold values from -0.15625 to 0.15625
- plane_coupling: bfloat16 [4, 8, 8], P('gx'), may hold values from -1 to 1
- face_owner: int32 [4, 8], P('gx'), may hold values from 0 to 7, each once within a row
Outputs:
- new_traces: bfloat16 [2, 4, 4, 2, 512, 768], P(None, 'gx', 'gy', 'gz')
The draws below stay inside these ranges and needn't reach their ends.
Inputs may be any that keep to these rules, and one draw needn't show every extreme that they name: `face_owner`: each row is a permutation of the 8 plane positions.
All inputs are finite; a program needn't handle non-finite values.
Results may differ from the reference program's by a relative error of at most 0.0062.
Values may be sent and summed in bfloat16 or wider, within the bound.
No kernel may reach another device: no remote copies, remote signals or barrier semaphores. Data moves between devices by JAX's collectives and lax.ppermute only.
A program may use at most 64 MiB of HBM per device.

```python
import jax
import jax.numpy as jnp
from jax import lax

W = 128
SLABS = 512
SWEEPS = 2
PLANE = 8
N_GX = 4
N_GY = 4
N_GZ = 2


def steps_of(rng, extent, cuts, low, top_value):
    def one(dim, shards_of):
        steps = jax.random.uniform(jax.random.fold_in(jax.random.fold_in(rng, 6), dim), (shards_of,), jnp.float32, low / len(cuts), top_value / len(cuts))
        return jnp.repeat(jnp.exp(steps), extent[dim] // shards_of).reshape((-1,) + (1,) * (len(extent) - dim - 1))

    loudness = one(*cuts[0])
    for cut in cuts[1:]:
        loudness = loudness * one(*cut)
    return loudness


def gaussian(stream_key, shape, spread, limit, split=(), dtype=jnp.bfloat16):
    array = spread * jax.random.normal(stream_key, shape, jnp.float32)
    if split:
        array = array * steps_of(stream_key, shape, split, -0.22, 0.18)
    return jnp.clip(array, -limit, limit).astype(dtype)


def setup_inputs(seed: int = 0) -> dict:
    keys = jax.random.split(jax.random.key(seed), 6)
    return {
        "traces": gaussian(keys[0], (2, N_GX, N_GY, N_GZ, SLABS, 6 * W), 1.0, 6.0, ((1, 4), (2, 4), (3, 2))),
        "sources": gaussian(keys[1], (2, N_GX, N_GY, N_GZ, SLABS, 6 * W), 0.5, 4.0, ((1, 4), (2, 4), (3, 2))),
        "local_ops": gaussian(keys[2], (2, N_GX, N_GY, N_GZ, 6 * W, 6 * W), (12 * W) ** -0.5, 0.15625, ((1, 4), (2, 4), (3, 2))),
        "plane_coupling": gaussian(keys[3], (N_GX, PLANE, PLANE), (4 * PLANE) ** -0.5, 1.0, ((0, 4),)),
        "face_owner": jax.vmap(lambda own: jax.random.permutation(own, PLANE))(jax.random.split(keys[4], N_GX)).reshape((N_GX, PLANE)).astype(jnp.int32),
    }


def solve_layer(layer_data):
    incoming, source_rows, operators = layer_data
    incoming = incoming.astype(jnp.float32)
    operators = operators.astype(jnp.float32)
    source_rows = source_rows.astype(jnp.float32)
    real_part = jnp.einsum('yzsc,yzcd->yzsd', incoming[0], operators[0]) - jnp.einsum('yzsc,yzcd->yzsd', incoming[1], operators[1]) + source_rows[0]
    imag_part = jnp.einsum('yzsc,yzcd->yzsd', incoming[0], operators[1]) + jnp.einsum('yzsc,yzcd->yzsd', incoming[1], operators[0]) + source_rows[1]
    return jnp.stack([real_part, imag_part]).astype(jnp.bfloat16)


def transmit(outgoing):
    face_view = outgoing.reshape(outgoing.shape[:5] + (6, W))
    moved_faces = []
    for dim_index in range(3):
        mesh_dim = 1 + dim_index
        lower_face = face_view[:, :, :, :, :, 2 * dim_index]
        upper_face = face_view[:, :, :, :, :, 2 * dim_index + 1]
        moved_faces.append(jnp.roll(upper_face, 1, axis=mesh_dim))
        moved_faces.append(jnp.roll(lower_face, -1, axis=mesh_dim))
    return jnp.stack(moved_faces, axis=5).reshape(outgoing.shape)


def couple_layer(layer_data):
    received, coupling, owners = layer_data
    picked = jnp.take(received, owners, axis=1).astype(jnp.float32)
    coupled = jnp.einsum('pq,rqsc->rpsc', coupling.astype(jnp.float32), picked)
    return (received.astype(jnp.float32) - coupled).astype(jnp.bfloat16)


def reference(traces, sources, local_ops, plane_coupling, face_owner):
    plane_size = N_GY * N_GZ
    incoming = traces
    source_view = jnp.moveaxis(sources, 1, 0)
    operator_view = jnp.moveaxis(local_ops, 1, 0)
    for sweep_step in range(SWEEPS):
        outgoing = lax.map(solve_layer, (jnp.moveaxis(incoming, 1, 0), source_view, operator_view))
        outgoing = jnp.moveaxis(outgoing, 0, 1)
        received = transmit(outgoing)
        stacked = jnp.moveaxis(received.reshape(2, N_GX, plane_size, SLABS, 6 * W), 1, 0)
        updated = lax.map(couple_layer, (stacked, plane_coupling, face_owner))
        incoming = jnp.moveaxis(updated, 0, 1).reshape(traces.shape)
    return incoming
```

```python
import functools

import jax
import jax.numpy as jnp
from jax import lax
from jax.experimental import pallas as pl
from jax.experimental.pallas import tpu as pltpu
from jax.sharding import PartitionSpec as P

SWEEPS = 2


def with_halo(block, sides, width):
    for axis, dim in sides:
        count = lax.axis_size(axis)
        forward = [(i, i + 1) for i in range(count - 1)]
        forward.append((count - 1, 0))
        backward = [(target, source) for source, target in forward]
        low = lax.ppermute(
            lax.slice_in_dim(block, block.shape[dim] - width, None, axis=dim), axis, forward
        )
        high = lax.ppermute(lax.slice_in_dim(block, 0, width, axis=dim), axis, backward)
        block = jnp.concatenate([low, block, high], axis=dim)
    return block


def many_subdomains(traces, sources, local_ops, plane_coupling, face_owner):
    columns_all = local_ops.shape[-1]
    slab_width = columns_all // 6
    slab_rows = traces.shape[4]
    count_y = lax.axis_size("gy")
    count_z = lax.axis_size("gz")
    plane_size = count_y * count_z
    block_rows_count = slab_rows // plane_size
    operators = local_ops.reshape(2, columns_all, columns_all)
    source_rows = sources.reshape(2, slab_rows, columns_all).astype(jnp.float32)
    incoming = traces.reshape(2, slab_rows, columns_all)
    owners = face_owner.reshape(plane_size)
    select = (owners[:, None] == jnp.arange(plane_size, dtype=jnp.int32)[None, :]).astype(
        jnp.float32
    )
    mixing = jnp.dot(
        plane_coupling.reshape(plane_size, plane_size).astype(jnp.float32),
        select,
        precision=lax.Precision.HIGHEST,
    ).astype(jnp.bfloat16)
    for _ in range(SWEEPS):
        real_part = (
            jnp.dot(incoming[0], operators[0], preferred_element_type=jnp.float32)
            - jnp.dot(incoming[1], operators[1], preferred_element_type=jnp.float32)
            + source_rows[0]
        )
        imag_part = (
            jnp.dot(incoming[0], operators[1], preferred_element_type=jnp.float32)
            + jnp.dot(incoming[1], operators[0], preferred_element_type=jnp.float32)
            + source_rows[1]
        )
        outgoing = (
            jnp.stack([real_part, imag_part])
            .astype(jnp.bfloat16)
            .reshape(2, slab_rows, 6, slab_width)
        )
        along_x = with_halo(outgoing[:, :, 0:2, :], (("gx", 2),), 1)
        partial_faces = jnp.concatenate(
            [along_x[:, :, 0:1], along_x[:, :, 3:4], outgoing[:, :, 2:6]], axis=2
        )
        blocks = partial_faces.reshape(2, plane_size, block_rows_count, 6, slab_width)
        update_block_rows = lax.all_to_all(
            blocks, ("gy", "gz"), split_axis=1, concat_axis=1, tiled=True
        )
        row_count = update_block_rows.shape[2]
        grid_view = update_block_rows.reshape(2, count_y, count_z, row_count, 6, slab_width)
        moved = jnp.stack(
            [
                grid_view[:, :, :, :, 0],
                grid_view[:, :, :, :, 1],
                jnp.roll(grid_view[:, :, :, :, 3], 1, axis=1),
                jnp.roll(grid_view[:, :, :, :, 2], -1, axis=1),
                jnp.roll(grid_view[:, :, :, :, 5], 1, axis=2),
                jnp.roll(grid_view[:, :, :, :, 4], -1, axis=2),
            ],
            axis=4,
        )
        block_rows = moved.reshape(2, plane_size, row_count * columns_all)
        coupled = jnp.einsum("pq,rqc->rpc", mixing, block_rows, preferred_element_type=jnp.float32)
        updated = (block_rows.astype(jnp.float32) - coupled).astype(jnp.bfloat16)
        updated = updated.reshape(2, plane_size, row_count, 6, slab_width)
        returned = lax.all_to_all(updated, ("gy", "gz"), split_axis=1, concat_axis=1, tiled=True)
        incoming = returned.reshape(2, slab_rows, columns_all)
    return incoming.reshape(traces.shape)


CHUNKS = 2
VMEM = pl.BlockSpec(memory_space=pltpu.VMEM)
SMEM = pl.BlockSpec(memory_space=pltpu.SMEM)


def plane_position():
    return lax.axis_index("gy") * lax.axis_size("gz") + lax.axis_index("gz")


def call(kernel, in_specs, out_shape, flops, out_specs=None, aliases=None):
    return pl.pallas_call(
        kernel,
        in_specs=in_specs,
        out_shape=out_shape,
        out_specs=out_specs if out_specs is not None else jax.tree.map(lambda _: VMEM, out_shape),
        input_output_aliases=aliases or {},
        cost_estimate=pl.CostEstimate(flops=flops, bytes_accessed=1 << 20, transcendentals=0),
        compiler_params=pltpu.CompilerParams(vmem_limit_bytes=32 << 20),
    )


def solve_rows(real, imag, operators_ref, source_of, outputs):
    real_part = jnp.dot(real, operators_ref[0], preferred_element_type=jnp.float32) - jnp.dot(
        imag, operators_ref[1], preferred_element_type=jnp.float32
    )
    imag_part = jnp.dot(real, operators_ref[1], preferred_element_type=jnp.float32) + jnp.dot(
        imag, operators_ref[0], preferred_element_type=jnp.float32
    )
    rows = outputs[0].shape[1]
    for part, result in enumerate((real_part, imag_part)):
        for k, output in enumerate(outputs):
            block = result[k * rows : (k + 1) * rows] + source_of(part, k)
            output[part] = block.astype(output.dtype)


def row_start(chunk, k, plane_size, rows):
    return pl.multiple_of((chunk * plane_size + (plane_position() ^ k)) * rows, rows)


def first_solve(chunk, plane_size, rows, traces_ref, sources_ref, operators_ref, *outputs):
    starts = [row_start(chunk, k, plane_size, rows) for k in range(plane_size)]
    real, imag = (
        jnp.concatenate([traces_ref[part, pl.ds(s, rows), :] for s in starts], axis=0)
        for part in range(2)
    )
    solve_rows(
        real,
        imag,
        operators_ref,
        lambda part, k: sources_ref[part, pl.ds(starts[k], rows), :].astype(jnp.float32),
        outputs,
    )


def next_solve(chunk, plane_size, rows, *refs):
    blocks, (sources_ref, operators_ref) = refs[:plane_size], refs[plane_size : plane_size + 2]
    starts = [row_start(chunk, k, plane_size, rows) for k in range(plane_size)]
    real, imag = (jnp.concatenate([b[part] for b in blocks], axis=0) for part in range(2))
    solve_rows(
        real,
        imag,
        operators_ref,
        lambda part, k: sources_ref[part, pl.ds(starts[k], rows), :].astype(jnp.float32),
        refs[plane_size + 2 :],
    )


def gather_x_faces(plane_size, width, *refs):
    blocks, (low_ref, high_ref) = refs[:plane_size], refs[plane_size:]
    for k, block in enumerate(blocks):
        low_ref[k] = block[:, :, 0:width]
        high_ref[k] = block[:, :, width : 2 * width]


def make_weights(count_y, count_z, coupling_ref, owner_ref, weights_ref, column_ref):
    plane_size = count_y * count_z
    me = plane_position()

    def clear(q, carry):
        for p in range(plane_size):
            column_ref[p, q] = jnp.where(p == q, jnp.float32(1), jnp.float32(0))
        return carry

    def couple(q, carry):
        owner = owner_ref[q]
        for p in range(plane_size):
            column_ref[p, owner] = column_ref[p, owner] - coupling_ref[p, q]
        return carry

    lax.fori_loop(0, plane_size, clear, 0)
    lax.fori_loop(0, plane_size, couple, 0)

    def fill(m, carry):
        source = me ^ m
        y, z = source // count_z, source % count_z
        receivers = (
            source,
            ((y + 1) % count_y) * count_z + z,
            ((y + count_y - 1) % count_y) * count_z + z,
            y * count_z + (z + 1) % count_z,
            y * count_z + (z + count_z - 1) % count_z,
        )
        for face, receiver in enumerate(receivers):
            for k in range(plane_size):
                weights_ref[face, k, m] = column_ref[me ^ k, receiver]
        return carry

    lax.fori_loop(0, plane_size, fill, 0)


def mix_blocks(plane_size, width, *refs):
    blocks = refs[:plane_size]
    from_low_ref, from_high_ref, weights_ref = refs[plane_size : plane_size + 3]
    outputs = refs[plane_size + 3 :]
    plan = ((0, None), (0, None), (1, 3), (2, 2), (3, 5), (4, 4))
    for face, (kind, source_face) in enumerate(plan):
        for part in range(2):
            if source_face is None:
                arrived = (from_low_ref, from_high_ref)[face]
                values = [arrived[m, part].astype(jnp.float32) for m in range(plane_size)]
            else:
                columns = slice(source_face * width, (source_face + 1) * width)
                values = [b[part, :, columns].astype(jnp.float32) for b in blocks]
            for k, output in enumerate(outputs):
                total = values[0] * weights_ref[kind, k, 0]
                for m in range(1, plane_size):
                    total = total + values[m] * weights_ref[kind, k, m]
                output[part, :, face * width : (face + 1) * width] = total.astype(output.dtype)


def store_rows(chunks, plane_size, rows, *refs):
    blocks, out_ref, sems = refs[: chunks * plane_size], refs[-2], refs[-1]
    copies = []
    for chunk in range(chunks):
        for k in range(plane_size):
            index = chunk * plane_size + k
            copies.append(
                pltpu.make_async_copy(
                    blocks[index],
                    out_ref.at[:, pl.ds(row_start(chunk, k, plane_size, rows), rows), :],
                    sems.at[index],
                )
            )
    for copy in copies:
        copy.start()
    for copy in copies:
        copy.wait()


def exchange(blocks, count_y, count_z):
    plane_size = count_y * count_z
    across = sorted(range(1, plane_size), key=lambda k: (-((k // count_z) // 2 > 0), k % count_z, k))
    received = [blocks[0]] + [None] * (plane_size - 1)
    for k in across:
        received[k] = lax.ppermute(blocks[k], ("gy", "gz"), [(p, p ^ k) for p in range(plane_size)])
    return received


def few_subdomains(traces, sources, local_ops, plane_coupling, face_owner):
    columns_all = local_ops.shape[-1]
    width = columns_all // 6
    slab_rows = traces.shape[4]
    count_x, count_y, count_z = (lax.axis_size(a) for a in ("gx", "gy", "gz"))
    plane_size = count_y * count_z
    rows = slab_rows // (plane_size * CHUNKS)
    operators = local_ops.reshape(2, columns_all, columns_all)
    source_rows = sources.reshape(2, slab_rows, columns_all)
    trace_rows = traces.reshape(2, slab_rows, columns_all)
    block = jax.ShapeDtypeStruct((2, rows, columns_all), traces.dtype)
    face = jax.ShapeDtypeStruct((plane_size, 2, rows, width), traces.dtype)
    solve_flops = 8 * plane_size * rows * columns_all * columns_all
    forward = [(i, (i + 1) % count_x) for i in range(count_x)]
    backward = [(target, source) for source, target in forward]

    weights = pl.pallas_call(
        functools.partial(make_weights, count_y, count_z),
        in_specs=[SMEM, SMEM],
        out_specs=SMEM,
        out_shape=jax.ShapeDtypeStruct((5, plane_size, plane_size), jnp.float32),
        scratch_shapes=[pltpu.SMEM((plane_size, plane_size), jnp.float32)],
    )(
        plane_coupling.reshape(plane_size, plane_size).astype(jnp.float32),
        face_owner.reshape(plane_size),
    )
    incoming = [None] * CHUNKS
    for sweep in range(SWEEPS):
        gathered = []
        for chunk in range(CHUNKS):
            if sweep == 0:
                outgoing = call(
                    functools.partial(first_solve, chunk, plane_size, rows),
                    [VMEM] * 3,
                    [block] * plane_size,
                    solve_flops,
                )(trace_rows, source_rows, operators)
            else:
                outgoing = call(
                    functools.partial(next_solve, chunk, plane_size, rows),
                    [VMEM] * (plane_size + 2),
                    [block] * plane_size,
                    solve_flops,
                )(*incoming[chunk], source_rows, operators)
            gathered.append(exchange(outgoing, count_y, count_z))
        for chunk in range(CHUNKS):
            low, high = call(
                functools.partial(gather_x_faces, plane_size, width),
                [VMEM] * plane_size,
                [face] * 2,
                solve_flops // 4,
            )(*gathered[chunk])
            from_low = lax.ppermute(high, "gx", forward)
            from_high = lax.ppermute(low, "gx", backward)
            updated = call(
                functools.partial(mix_blocks, plane_size, width),
                [VMEM] * (plane_size + 2) + [SMEM],
                [block] * plane_size,
                solve_flops,
            )(*gathered[chunk], from_low, from_high, weights)
            incoming[chunk] = exchange(updated, count_y, count_z)
    result = pl.pallas_call(
        functools.partial(store_rows, CHUNKS, plane_size, rows),
        in_specs=[VMEM] * (CHUNKS * plane_size),
        out_specs=pl.BlockSpec(memory_space=pl.ANY),
        out_shape=jax.ShapeDtypeStruct((2, slab_rows, columns_all), traces.dtype),
        scratch_shapes=[pltpu.SemaphoreType.DMA((CHUNKS * plane_size,))],
    )(*(b for chunk in incoming for b in chunk))
    return result.reshape(traces.shape)


def solution(mesh):
    placed = (
        P(None, "gx", "gy", "gz", None, None),
        P(None, "gx", "gy", "gz", None, None),
        P(None, "gx", "gy", "gz", None, None),
        P("gx", None, None),
        P("gx", None),
    )
    few = mesh.shape["gy"] * mesh.shape["gz"] <= 8
    return jax.shard_map(
        few_subdomains if few else many_subdomains,
        mesh=mesh,
        in_specs=placed,
        out_specs=P(None, "gx", "gy", "gz", None, None),
        check_vma=False,
    )
```

```python
import functools

import jax
import jax.numpy as jnp
from jax import lax
from jax.experimental import pallas as pl
from jax.experimental.pallas import tpu as pltpu
from jax.sharding import PartitionSpec as P

SWEEPS = 2


def with_halo(block, sides, width):
    for axis, dim in sides:
        count = lax.axis_size(axis)
        forward = [(i, i + 1) for i in range(count - 1)]
        forward.append((count - 1, 0))
        backward = [(target, source) for source, target in forward]
        low = lax.ppermute(
            lax.slice_in_dim(block, block.shape[dim] - width, None, axis=dim), axis, forward
        )
        high = lax.ppermute(lax.slice_in_dim(block, 0, width, axis=dim), axis, backward)
        block = jnp.concatenate([low, block, high], axis=dim)
    return block


def many_subdomains(traces, sources, local_ops, plane_coupling, face_owner):
    columns_all = local_ops.shape[-1]
    slab_width = columns_all // 6
    slab_rows = traces.shape[4]
    count_y = lax.axis_size("gy")
    count_z = lax.axis_size("gz")
    plane_size = count_y * count_z
    block_rows_count = slab_rows // plane_size
    operators = local_ops.reshape(2, columns_all, columns_all)
    source_rows = sources.reshape(2, slab_rows, columns_all).astype(jnp.float32)
    incoming = traces.reshape(2, slab_rows, columns_all)
    owners = face_owner.reshape(plane_size)
    select = (owners[:, None] == jnp.arange(plane_size, dtype=jnp.int32)[None, :]).astype(
        jnp.float32
    )
    mixing = jnp.dot(
        plane_coupling.reshape(plane_size, plane_size).astype(jnp.float32),
        select,
        precision=lax.Precision.HIGHEST,
    ).astype(jnp.bfloat16)
    for _ in range(SWEEPS):
        real_part = (
            jnp.dot(incoming[0], operators[0], preferred_element_type=jnp.float32)
            - jnp.dot(incoming[1], operators[1], preferred_element_type=jnp.float32)
            + source_rows[0]
        )
        imag_part = (
            jnp.dot(incoming[0], operators[1], preferred_element_type=jnp.float32)
            + jnp.dot(incoming[1], operators[0], preferred_element_type=jnp.float32)
            + source_rows[1]
        )
        outgoing = (
            jnp.stack([real_part, imag_part])
            .astype(jnp.bfloat16)
            .reshape(2, slab_rows, 6, slab_width)
        )
        along_x = with_halo(outgoing[:, :, 0:2, :], (("gx", 2),), 1)
        partial_faces = jnp.concatenate(
            [along_x[:, :, 0:1], along_x[:, :, 3:4], outgoing[:, :, 2:6]], axis=2
        )
        blocks = partial_faces.reshape(2, plane_size, block_rows_count, 6, slab_width)
        update_block_rows = lax.all_to_all(
            blocks, ("gy", "gz"), split_axis=1, concat_axis=1, tiled=True
        )
        row_count = update_block_rows.shape[2]
        grid_view = update_block_rows.reshape(2, count_y, count_z, row_count, 6, slab_width)
        moved = jnp.stack(
            [
                grid_view[:, :, :, :, 0],
                grid_view[:, :, :, :, 1],
                jnp.roll(grid_view[:, :, :, :, 3], 1, axis=1),
                jnp.roll(grid_view[:, :, :, :, 2], -1, axis=1),
                jnp.roll(grid_view[:, :, :, :, 5], 1, axis=2),
                jnp.roll(grid_view[:, :, :, :, 4], -1, axis=2),
            ],
            axis=4,
        )
        block_rows = moved.reshape(2, plane_size, row_count * columns_all)
        coupled = jnp.einsum("pq,rqc->rpc", mixing, block_rows, preferred_element_type=jnp.float32)
        updated = (block_rows.astype(jnp.float32) - coupled).astype(jnp.bfloat16)
        updated = updated.reshape(2, plane_size, row_count, 6, slab_width)
        returned = lax.all_to_all(updated, ("gy", "gz"), split_axis=1, concat_axis=1, tiled=True)
        incoming = returned.reshape(2, slab_rows, columns_all)
    return incoming.reshape(traces.shape)


VMEM = pl.BlockSpec(memory_space=pltpu.VMEM)
SMEM = pl.BlockSpec(memory_space=pltpu.SMEM)
HBM = pl.BlockSpec(memory_space=pltpu.HBM)
KERNEL_BYTES = 24 << 20
FIRST_BYTES = 50 << 20
KERNEL_FLOPS = 1 << 31


def plane_position():
    return lax.axis_index("gy") * lax.axis_size("gz") + lax.axis_index("gz")


def call(kernel, in_specs, out_shape, out_specs=None, aliases=None, scratch=(), limit=KERNEL_BYTES):
    return pl.pallas_call(
        kernel,
        in_specs=in_specs,
        out_shape=out_shape,
        out_specs=out_specs if out_specs is not None else jax.tree.map(lambda _: VMEM, out_shape),
        scratch_shapes=scratch,
        input_output_aliases=aliases or {},
        cost_estimate=pl.CostEstimate(
            flops=KERNEL_FLOPS, bytes_accessed=1 << 20, transcendentals=0
        ),
        compiler_params=pltpu.CompilerParams(vmem_limit_bytes=limit),
    )


def row_start(k, rows):
    return pl.multiple_of((plane_position() ^ k) * rows, rows)


def part_products(part, real, imag, operators):
    if part == 0:
        return jnp.dot(real, operators[0], preferred_element_type=jnp.float32) - jnp.dot(
            imag, operators[1], preferred_element_type=jnp.float32
        )
    return jnp.dot(real, operators[1], preferred_element_type=jnp.float32) + jnp.dot(
        imag, operators[0], preferred_element_type=jnp.float32
    )


def load_and_solve(ks, plane_size, rows, first, columns, traces_ref, sources_ref, operators_ref, *refs):
    blocks, (traces, sources, operators, sems) = refs[: len(ks)], refs[len(ks) :]
    wanted = [slice(first, first + columns)]
    unwanted = [slice(0, first), slice(first + columns, operators.shape[-1])]
    unwanted = [c for c in unwanted if c.stop > c.start]
    others = [k for k in range(plane_size) if k not in ks]

    def rows_of(source, target, which):
        return [
            (source.at[:, pl.ds(row_start(k, rows), rows), :], target.at[k]) for k in which
        ]

    def operators_of(which):
        return [
            (operators_ref.at[part, :, c], operators.at[part, :, c])
            for c in which
            for part in range(2)
        ]

    needed = rows_of(traces_ref, traces, ks) + operators_of(wanted)
    late = rows_of(sources_ref, sources, ks)
    rest = rows_of(traces_ref, traces, others) + operators_of(unwanted)
    rest += rows_of(sources_ref, sources, others)
    copies = [
        pltpu.make_async_copy(source, target, sems.at[n])
        for n, (source, target) in enumerate(needed + late + rest)
    ]
    for copy in copies:
        copy.start()
    for copy in copies[: len(needed)]:
        copy.wait()
    real, imag = (jnp.concatenate([traces[k, part] for k in ks], axis=0) for part in range(2))
    results = [
        part_products(part, real, imag, [operators[p, :, wanted[0]] for p in range(2)])
        for part in range(2)
    ]
    for copy in copies[len(needed) : len(needed) + len(late)]:
        copy.wait()
    finish(ks, rows, wanted[0], pick_block, results, sources, blocks)
    for copy in copies[len(needed) + len(late) :]:
        copy.wait()


def finish(ks, rows, wanted, pick, results, sources, outputs):
    for part, result in enumerate(results):
        for n, k in enumerate(ks):
            block = result[n * rows : (n + 1) * rows] + sources[k, part, :, wanted].astype(
                jnp.float32
            )
            pick(outputs, part, n, block.astype(outputs[0].dtype))


def solve_blocks(ks, rows, first, columns, pick, count, *refs):
    wanted = slice(first, first + columns)
    if count == 1:
        traces, sources, operators_ref = refs[:3]
        outputs = refs[3:]
        pieces = [[jnp.concatenate([traces[k, part] for k in ks], axis=0) for part in range(2)]]
    else:
        incoming, (sources, operators_ref) = refs[: 2 * len(ks)], refs[2 * len(ks) : 2 * len(ks) + 2]
        outputs = refs[2 * len(ks) + 2 :]
        pieces = [
            [jnp.concatenate([b[part] for b in group], axis=0) for part in range(2)]
            for group in (incoming[: len(ks)], incoming[len(ks) :])
        ]
    results = [0.0, 0.0]
    start = 0
    for real, imag in pieces:
        depth = slice(start, start + real.shape[-1])
        start = depth.stop
        operators = [operators_ref[part, depth, wanted] for part in range(2)]
        for part in range(2):
            results[part] = results[part] + part_products(part, real, imag, operators)
    finish(ks, rows, wanted, pick, results, sources, outputs)


def pick_block(outputs, part, k, block):
    outputs[k][part] = block


def pick_face(outputs, part, k, block):
    width = block.shape[-1] // 2
    outputs[0][k, part] = block[:, :width]
    outputs[1][k, part] = block[:, width:]


def pack_faces(from_low_ref, from_high_ref, *outputs):
    width = from_low_ref.shape[-1]
    for k, output in enumerate(outputs):
        output[:, :, :width] = from_low_ref[k]
        output[:, :, width:] = from_high_ref[k]


def make_weights(count_y, count_z, coupling_ref, owner_ref, weights_ref, column_ref):
    plane_size = count_y * count_z
    me = plane_position()

    def clear(q, carry):
        for p in range(plane_size):
            column_ref[p, q] = jnp.where(p == q, jnp.float32(1), jnp.float32(0))
        return carry

    def couple(q, carry):
        owner = owner_ref[q]
        for p in range(plane_size):
            column_ref[p, owner] = column_ref[p, owner] - coupling_ref[p, q]
        return carry

    lax.fori_loop(0, plane_size, clear, 0)
    lax.fori_loop(0, plane_size, couple, 0)

    def fill(m, carry):
        source = me ^ m
        y, z = source // count_z, source % count_z
        receivers = (
            source,
            ((y + 1) % count_y) * count_z + z,
            ((y + count_y - 1) % count_y) * count_z + z,
            y * count_z + (z + 1) % count_z,
            y * count_z + (z + count_z - 1) % count_z,
        )
        for face, receiver in enumerate(receivers):
            for k in range(plane_size):
                weights_ref[face, k, m] = column_ref[me ^ k, receiver]
        return carry

    lax.fori_loop(0, plane_size, fill, 0)


def mix_blocks(plane_size, plan, *refs):
    blocks, weights_ref, outputs = refs[:plane_size], refs[plane_size], refs[plane_size + 1 :]
    width = blocks[0].shape[-1] // len(plan)
    for face, (kind, source_face) in enumerate(plan):
        columns = slice(source_face * width, (source_face + 1) * width)
        for part in range(2):
            values = [b[part, :, columns].astype(jnp.float32) for b in blocks]
            for k, output in enumerate(outputs):
                total = values[0] * weights_ref[kind, k, 0]
                for m in range(1, plane_size):
                    total = total + values[m] * weights_ref[kind, k, m]
                output[part, :, face * width : (face + 1) * width] = total.astype(output.dtype)


def store_rows(plane_size, rows, first, *refs):
    blocks, out_ref, sems = refs[:plane_size], refs[-2], refs[-1]
    columns = blocks[0].shape[-1]
    copies = [
        pltpu.make_async_copy(
            blocks[k],
            out_ref.at[:, pl.ds(row_start(k, rows), rows), pl.ds(first, columns)],
            sems.at[k],
        )
        for k in range(plane_size)
    ]
    for copy in copies:
        copy.start()
    for copy in copies:
        copy.wait()


def partners(count_y, count_z):
    across = range(1, count_y * count_z)
    return sorted(across, key=lambda k: (2 * (k // count_z) < count_y, k % count_z, k))


def far_and_near(count_y, count_z):
    ks = partners(count_y, count_z)
    far = tuple(k for k in ks if 2 * (k // count_z) >= count_y)
    return far, tuple(k for k in ks if k not in far)


def row_groups(count_y, count_z):
    far, near = far_and_near(count_y, count_z)
    half = len(far) // 2
    return [ks for ks in (far[:half], far[half:], (0,) + near) if ks]


def exchange(blocks, count_y, count_z):
    plane_size = count_y * count_z
    received = [blocks[0]] + [None] * (plane_size - 1)
    for k in partners(count_y, count_z):
        received[k] = lax.ppermute(blocks[k], ("gy", "gz"), [(p, p ^ k) for p in range(plane_size)])
    return received


def few_subdomains(traces, sources, local_ops, plane_coupling, face_owner):
    columns_all = local_ops.shape[-1]
    width = columns_all // 6
    slab_rows = traces.shape[4]
    count_x, count_y, count_z = (lax.axis_size(a) for a in ("gx", "gy", "gz"))
    plane_size = count_y * count_z
    rows = slab_rows // plane_size
    operators = local_ops.reshape(2, columns_all, columns_all)
    source_rows = sources.reshape(2, slab_rows, columns_all)
    trace_rows = traces.reshape(2, slab_rows, columns_all)
    dtype = traces.dtype
    forward = [(i, (i + 1) % count_x) for i in range(count_x)]
    backward = [(target, source) for source, target in forward]
    whole = jax.ShapeDtypeStruct((2, slab_rows, columns_all), dtype)
    groups = {"x": (0, 2 * width), "yz": (2 * width, 4 * width)}
    plans = {"x": ((0, 0), (0, 1)), "yz": ((1, 1), (2, 0), (3, 3), (4, 2))}
    face = jax.ShapeDtypeStruct((plane_size, 2, rows, width), dtype)
    blocks_of = {
        g: [jax.ShapeDtypeStruct((2, rows, columns), dtype)] * plane_size
        for g, (_, columns) in groups.items()
    }
    solved = {"x": ([face] * 2, pick_face), "yz": (blocks_of["yz"], pick_block)}

    placed = []

    def solve(group, sweep, ks, incoming):
        first, columns = groups[group]
        out_shape, pick = solved[group]
        if group == "yz":
            out_shape = out_shape[: len(ks)]
        if not placed:
            by_block = jax.ShapeDtypeStruct((plane_size, 2, rows, columns_all), dtype)
            results = call(
                functools.partial(load_and_solve, ks, plane_size, rows, first, columns),
                [HBM] * 3,
                out_shape
                + [by_block, by_block, jax.ShapeDtypeStruct(operators.shape, dtype)],
                scratch=[pltpu.SemaphoreType.DMA((2 * plane_size + 6,))],
                limit=FIRST_BYTES,
            )(trace_rows, source_rows, operators)
            placed.extend(results[len(ks) :])
            return results[: len(ks)]
        if sweep == 0:
            arrays = [placed[0]]
        else:
            arrays = [incoming[g][k] for g in ("x", "yz") for k in ks]
        return call(
            functools.partial(solve_blocks, ks, rows, first, columns, pick, 1 if sweep == 0 else 2),
            [VMEM] * (len(arrays) + 2),
            out_shape,
        )(*arrays, *placed[1:])

    def mix(group, gathered, weights):
        return call(
            functools.partial(mix_blocks, plane_size, plans[group]),
            [VMEM] * plane_size + [SMEM],
            blocks_of[group],
        )(*gathered, weights)

    def store(group, blocks, so_far):
        before = [] if so_far is None else [so_far]
        return call(
            functools.partial(store_rows, plane_size, rows, groups[group][0]),
            [VMEM] * plane_size + [HBM] * len(before),
            whole,
            out_specs=HBM,
            aliases={plane_size: 0} if before else None,
            scratch=[pltpu.SemaphoreType.DMA((plane_size,))],
        )(*blocks, *before)

    weights = call(
        functools.partial(make_weights, count_y, count_z),
        [SMEM, SMEM],
        jax.ShapeDtypeStruct((5, plane_size, plane_size), jnp.float32),
        out_specs=SMEM,
        scratch=[pltpu.SMEM((plane_size, plane_size), jnp.float32)],
    )(
        plane_coupling.reshape(plane_size, plane_size).astype(jnp.float32),
        face_owner.reshape(plane_size),
    )
    incoming = None
    for sweep in range(SWEEPS):
        out_yz = [None] * plane_size
        for ks in row_groups(count_y, count_z):
            for k, block in zip(ks, solve("yz", sweep, ks, incoming)):
                out_yz[k] = block
        gathered_yz = exchange(out_yz, count_y, count_z)
        low, high = solve("x", sweep, tuple(range(plane_size)), incoming)
        from_low = lax.ppermute(high, "gx", forward)
        from_high = lax.ppermute(low, "gx", backward)
        packed = call(pack_faces, [VMEM] * 2, blocks_of["x"])(from_low, from_high)
        gathered_x = exchange(packed, count_y, count_z)
        mixed_yz = mix("yz", gathered_yz, weights)
        incoming = {"yz": exchange(mixed_yz, count_y, count_z)}
        mixed_x = mix("x", gathered_x, weights)
        incoming["x"] = exchange(mixed_x, count_y, count_z)
    result = store("x", incoming["x"], store("yz", incoming["yz"], None))
    return result.reshape(traces.shape)


def solution(mesh):
    placed = (
        P(None, "gx", "gy", "gz", None, None),
        P(None, "gx", "gy", "gz", None, None),
        P(None, "gx", "gy", "gz", None, None),
        P("gx", None, None),
        P("gx", None),
    )
    counts = [mesh.shape[a] for a in ("gy", "gz")]
    few = counts[0] * counts[1] <= 8 and all(c & (c - 1) == 0 for c in counts)
    return jax.shard_map(
        few_subdomains if few else many_subdomains,
        mesh=mesh,
        in_specs=placed,
        out_specs=P(None, "gx", "gy", "gz", None, None),
        check_vma=False,
    )
```

```python
import functools

import jax
import jax.numpy as jnp
from jax import lax
from jax.experimental import pallas as pl
from jax.experimental.pallas import tpu as pltpu
from jax.sharding import PartitionSpec as P

SWEEPS = 2


def with_halo(block, sides, width):
    for axis, dim in sides:
        count = lax.axis_size(axis)
        forward = [(i, i + 1) for i in range(count - 1)]
        forward.append((count - 1, 0))
        backward = [(target, source) for source, target in forward]
        low = lax.ppermute(
            lax.slice_in_dim(block, block.shape[dim] - width, None, axis=dim), axis, forward
        )
        high = lax.ppermute(lax.slice_in_dim(block, 0, width, axis=dim), axis, backward)
        block = jnp.concatenate([low, block, high], axis=dim)
    return block


def many_subdomains(traces, sources, local_ops, plane_coupling, face_owner):
    columns_all = local_ops.shape[-1]
    slab_width = columns_all // 6
    slab_rows = traces.shape[4]
    count_y = lax.axis_size("gy")
    count_z = lax.axis_size("gz")
    plane_size = count_y * count_z
    block_rows_count = slab_rows // plane_size
    operators = local_ops.reshape(2, columns_all, columns_all)
    source_rows = sources.reshape(2, slab_rows, columns_all).astype(jnp.float32)
    incoming = traces.reshape(2, slab_rows, columns_all)
    owners = face_owner.reshape(plane_size)
    select = (owners[:, None] == jnp.arange(plane_size, dtype=jnp.int32)[None, :]).astype(
        jnp.float32
    )
    mixing = jnp.dot(
        plane_coupling.reshape(plane_size, plane_size).astype(jnp.float32),
        select,
        precision=lax.Precision.HIGHEST,
    ).astype(jnp.bfloat16)
    for _ in range(SWEEPS):
        real_part = (
            jnp.dot(incoming[0], operators[0], preferred_element_type=jnp.float32)
            - jnp.dot(incoming[1], operators[1], preferred_element_type=jnp.float32)
            + source_rows[0]
        )
        imag_part = (
            jnp.dot(incoming[0], operators[1], preferred_element_type=jnp.float32)
            + jnp.dot(incoming[1], operators[0], preferred_element_type=jnp.float32)
            + source_rows[1]
        )
        outgoing = (
            jnp.stack([real_part, imag_part])
            .astype(jnp.bfloat16)
            .reshape(2, slab_rows, 6, slab_width)
        )
        along_x = with_halo(outgoing[:, :, 0:2, :], (("gx", 2),), 1)
        partial_faces = jnp.concatenate(
            [along_x[:, :, 0:1], along_x[:, :, 3:4], outgoing[:, :, 2:6]], axis=2
        )
        blocks = partial_faces.reshape(2, plane_size, block_rows_count, 6, slab_width)
        update_block_rows = lax.all_to_all(
            blocks, ("gy", "gz"), split_axis=1, concat_axis=1, tiled=True
        )
        row_count = update_block_rows.shape[2]
        grid_view = update_block_rows.reshape(2, count_y, count_z, row_count, 6, slab_width)
        moved = jnp.stack(
            [
                grid_view[:, :, :, :, 0],
                grid_view[:, :, :, :, 1],
                jnp.roll(grid_view[:, :, :, :, 3], 1, axis=1),
                jnp.roll(grid_view[:, :, :, :, 2], -1, axis=1),
                jnp.roll(grid_view[:, :, :, :, 5], 1, axis=2),
                jnp.roll(grid_view[:, :, :, :, 4], -1, axis=2),
            ],
            axis=4,
        )
        block_rows = moved.reshape(2, plane_size, row_count * columns_all)
        coupled = jnp.einsum("pq,rqc->rpc", mixing, block_rows, preferred_element_type=jnp.float32)
        updated = (block_rows.astype(jnp.float32) - coupled).astype(jnp.bfloat16)
        updated = updated.reshape(2, plane_size, row_count, 6, slab_width)
        returned = lax.all_to_all(updated, ("gy", "gz"), split_axis=1, concat_axis=1, tiled=True)
        incoming = returned.reshape(2, slab_rows, columns_all)
    return incoming.reshape(traces.shape)


VMEM = pl.BlockSpec(memory_space=pltpu.VMEM)
SMEM = pl.BlockSpec(memory_space=pltpu.SMEM)
HBM = pl.BlockSpec(memory_space=pltpu.HBM)
KERNEL_BYTES = 24 << 20
FIRST_BYTES = 53 << 20
LOAD_BYTES = 50 << 20
PIECES = 1
KERNEL_FLOPS = 1 << 31


def plane_position():
    return lax.axis_index("gy") * lax.axis_size("gz") + lax.axis_index("gz")


def call(kernel, in_specs, out_shape, out_specs=None, aliases=None, scratch=(), limit=KERNEL_BYTES):
    return pl.pallas_call(
        kernel,
        in_specs=in_specs,
        out_shape=out_shape,
        out_specs=out_specs if out_specs is not None else jax.tree.map(lambda _: VMEM, out_shape),
        scratch_shapes=scratch,
        input_output_aliases=aliases or {},
        cost_estimate=pl.CostEstimate(
            flops=KERNEL_FLOPS, bytes_accessed=1 << 20, transcendentals=0
        ),
        compiler_params=pltpu.CompilerParams(vmem_limit_bytes=limit),
    )


def row_start(k, rows):
    return pl.multiple_of((plane_position() ^ k) * rows, rows)


def part_products(part, real, imag, operators):
    if part == 0:
        return jnp.dot(real, operators[0], preferred_element_type=jnp.float32) - jnp.dot(
            imag, operators[1], preferred_element_type=jnp.float32
        )
    return jnp.dot(real, operators[1], preferred_element_type=jnp.float32) + jnp.dot(
        imag, operators[0], preferred_element_type=jnp.float32
    )


def start_all(pairs, sems):
    copies = [
        pltpu.make_async_copy(source, target, sems.at[n]) for n, (source, target) in enumerate(pairs)
    ]
    for copy in copies:
        copy.start()
    return copies


def load_and_solve(ks, rows, first, columns, traces_ref, sources_ref, operators_ref, *refs):
    blocks, operators, (traces, sources, sems) = refs[: len(ks)], refs[len(ks)], refs[-3:]
    wanted = pl.ds(first, columns)
    here = [pl.ds(row_start(k, rows), rows) for k in ks]
    depth = operators.shape[1] // PIECES
    depths = [slice(n * depth, (n + 1) * depth) for n in range(PIECES)]
    pairs = [(traces_ref.at[:, r, :], traces.at[n]) for n, r in enumerate(here)]
    for d in depths:
        for part in range(2):
            pairs.append((operators_ref.at[part, d, wanted], operators.at[part, d]))
    pairs += [(sources_ref.at[:, r, wanted], sources.at[n]) for n, r in enumerate(here)]
    copies = start_all(pairs, sems)
    rows_here, pieces, late = copies[: len(ks)], copies[len(ks) : -len(ks)], copies[-len(ks) :]
    for copy in rows_here:
        copy.wait()
    results = [0.0, 0.0]
    for n, d in enumerate(depths):
        for copy in pieces[2 * n : 2 * n + 2]:
            copy.wait()
        real, imag = (
            jnp.concatenate([traces[k, part, :, d] for k in range(len(ks))], axis=0)
            for part in range(2)
        )
        for part in range(2):
            results[part] = results[part] + part_products(
                part, real, imag, [operators[p, d] for p in range(2)]
            )
    for copy in late:
        copy.wait()
    finish(range(len(ks)), rows, slice(0, columns), pick_block, results, sources, blocks)


def load_rest(
    plane_size, rows, first, columns, traces_ref, sources_ref, operators_ref, traces, sources, operators, sems
):
    pairs = []
    for source, target in ((traces_ref, traces), (sources_ref, sources)):
        for k in range(plane_size):
            pairs.append((source.at[:, pl.ds(row_start(k, rows), rows), :], target.at[k]))
    pairs.append((operators_ref.at[:, :, pl.ds(first, columns)], operators))
    for copy in start_all(pairs, sems):
        copy.wait()


def finish(ks, rows, wanted, pick, results, sources, outputs):
    for part, result in enumerate(results):
        for n, k in enumerate(ks):
            block = result[n * rows : (n + 1) * rows] + sources[k, part, :, wanted].astype(
                jnp.float32
            )
            pick(outputs, part, n, block.astype(outputs[0].dtype))


def solve_blocks(ks, rows, first, columns, pick, count, *refs):
    wanted = slice(first, first + columns)
    if count == 1:
        traces, sources, operators_ref = refs[:3]
        outputs = refs[3:]
        pieces = [[jnp.concatenate([traces[k, part] for k in ks], axis=0) for part in range(2)]]
    else:
        incoming, (sources, operators_ref) = refs[: 2 * len(ks)], refs[2 * len(ks) : 2 * len(ks) + 2]
        outputs = refs[2 * len(ks) + 2 :]
        pieces = [
            [jnp.concatenate([b[part] for b in group], axis=0) for part in range(2)]
            for group in (incoming[: len(ks)], incoming[len(ks) :])
        ]
    results = [0.0, 0.0]
    start = 0
    for real, imag in pieces:
        depth = slice(start, start + real.shape[-1])
        start = depth.stop
        operators = [operators_ref[part, depth] for part in range(2)]
        for part in range(2):
            results[part] = results[part] + part_products(part, real, imag, operators)
    finish(ks, rows, wanted, pick, results, sources, outputs)


def pick_block(outputs, part, k, block):
    outputs[k][part] = block


def pick_face(outputs, part, k, block):
    width = block.shape[-1] // 2
    outputs[0][k, part] = block[:, :width]
    outputs[1][k, part] = block[:, width:]


def pack_faces(from_low_ref, from_high_ref, *outputs):
    width = from_low_ref.shape[-1]
    for k, output in enumerate(outputs):
        output[:, :, :width] = from_low_ref[k]
        output[:, :, width:] = from_high_ref[k]


def make_weights(count_y, count_z, coupling_ref, owner_ref, weights_ref, column_ref):
    plane_size = count_y * count_z
    me = plane_position()

    def clear(q, carry):
        for p in range(plane_size):
            column_ref[p, q] = jnp.where(p == q, jnp.float32(1), jnp.float32(0))
        return carry

    def couple(q, carry):
        owner = owner_ref[q]
        for p in range(plane_size):
            column_ref[p, owner] = column_ref[p, owner] - coupling_ref[p, q]
        return carry

    lax.fori_loop(0, plane_size, clear, 0)
    lax.fori_loop(0, plane_size, couple, 0)

    def fill(m, carry):
        source = me ^ m
        y, z = source // count_z, source % count_z
        receivers = (
            source,
            ((y + 1) % count_y) * count_z + z,
            ((y + count_y - 1) % count_y) * count_z + z,
            y * count_z + (z + 1) % count_z,
            y * count_z + (z + count_z - 1) % count_z,
        )
        for face, receiver in enumerate(receivers):
            for k in range(plane_size):
                weights_ref[face, k, m] = column_ref[me ^ k, receiver]
        return carry

    lax.fori_loop(0, plane_size, fill, 0)


def mix_blocks(plane_size, plan, *refs):
    blocks, weights_ref, outputs = refs[:plane_size], refs[plane_size], refs[plane_size + 1 :]
    width = blocks[0].shape[-1] // len(plan)
    for face, (kind, source_face) in enumerate(plan):
        columns = slice(source_face * width, (source_face + 1) * width)
        for part in range(2):
            values = [b[part, :, columns].astype(jnp.float32) for b in blocks]
            for k, output in enumerate(outputs):
                total = values[0] * weights_ref[kind, k, 0]
                for m in range(1, plane_size):
                    total = total + values[m] * weights_ref[kind, k, m]
                output[part, :, face * width : (face + 1) * width] = total.astype(output.dtype)


def store_rows(plane_size, rows, first, *refs):
    blocks, out_ref, sems = refs[:plane_size], refs[-2], refs[-1]
    columns = blocks[0].shape[-1]
    copies = [
        pltpu.make_async_copy(
            blocks[k],
            out_ref.at[:, pl.ds(row_start(k, rows), rows), pl.ds(first, columns)],
            sems.at[k],
        )
        for k in range(plane_size)
    ]
    for copy in copies:
        copy.start()
    for copy in copies:
        copy.wait()


def partners(count_y, count_z):
    across = range(1, count_y * count_z)
    return sorted(across, key=lambda k: (2 * (k // count_z) < count_y, k % count_z, k))


def far_and_near(count_y, count_z):
    ks = partners(count_y, count_z)
    far = tuple(k for k in ks if 2 * (k // count_z) >= count_y)
    return far, tuple(k for k in ks if k not in far)


def row_groups(count_y, count_z):
    far, near = far_and_near(count_y, count_z)
    half = len(far) // 2
    return [ks for ks in (far[:half], far[half:], (0,) + near) if ks]


def exchange(blocks, count_y, count_z):
    plane_size = count_y * count_z
    received = [blocks[0]] + [None] * (plane_size - 1)
    for k in partners(count_y, count_z):
        received[k] = lax.ppermute(blocks[k], ("gy", "gz"), [(p, p ^ k) for p in range(plane_size)])
    return received


def few_subdomains(traces, sources, local_ops, plane_coupling, face_owner):
    columns_all = local_ops.shape[-1]
    width = columns_all // 6
    slab_rows = traces.shape[4]
    count_x, count_y, count_z = (lax.axis_size(a) for a in ("gx", "gy", "gz"))
    plane_size = count_y * count_z
    rows = slab_rows // plane_size
    operators = local_ops.reshape(2, columns_all, columns_all)
    source_rows = sources.reshape(2, slab_rows, columns_all)
    trace_rows = traces.reshape(2, slab_rows, columns_all)
    dtype = traces.dtype
    forward = [(i, (i + 1) % count_x) for i in range(count_x)]
    backward = [(target, source) for source, target in forward]
    whole = jax.ShapeDtypeStruct((2, slab_rows, columns_all), dtype)
    groups = {"x": (0, 2 * width), "yz": (2 * width, 4 * width)}
    plans = {"x": ((0, 0), (0, 1)), "yz": ((1, 1), (2, 0), (3, 3), (4, 2))}
    face = jax.ShapeDtypeStruct((plane_size, 2, rows, width), dtype)
    blocks_of = {
        g: [jax.ShapeDtypeStruct((2, rows, columns), dtype)] * plane_size
        for g, (_, columns) in groups.items()
    }
    solved = {"x": ([face] * 2, pick_face), "yz": (blocks_of["yz"], pick_block)}

    placed = {}

    def solve(group, sweep, ks, incoming):
        first, columns = groups[group]
        out_shape, pick = solved[group]
        if group == "yz":
            out_shape = out_shape[: len(ks)]
        if not placed:
            *blocks, placed[group] = call(
                functools.partial(load_and_solve, ks, rows, first, columns),
                [HBM] * 3,
                out_shape + [jax.ShapeDtypeStruct((2, columns_all, columns), dtype)],
                scratch=[
                    pltpu.VMEM((len(ks), 2, rows, columns_all), dtype),
                    pltpu.VMEM((len(ks), 2, rows, columns), dtype),
                    pltpu.SemaphoreType.DMA((2 * len(ks) + 2 * PIECES,)),
                ],
                limit=FIRST_BYTES,
            )(trace_rows, source_rows, operators)
            return blocks
        if sweep == 0:
            arrays = [placed["traces"]]
        else:
            arrays = [incoming[g][k] for g in ("x", "yz") for k in ks]
        return call(
            functools.partial(solve_blocks, ks, rows, first, columns, pick, 1 if sweep == 0 else 2),
            [VMEM] * (len(arrays) + 2),
            out_shape,
        )(*arrays, placed["sources"], placed[group])

    def load():
        first, columns = groups["x"]
        by_block = jax.ShapeDtypeStruct((plane_size, 2, rows, columns_all), dtype)
        placed["traces"], placed["sources"], placed["x"] = call(
            functools.partial(load_rest, plane_size, rows, first, columns),
            [HBM] * 3,
            [by_block, by_block, jax.ShapeDtypeStruct((2, columns_all, columns), dtype)],
            scratch=[pltpu.SemaphoreType.DMA((2 * plane_size + 1,))],
            limit=LOAD_BYTES,
        )(trace_rows, source_rows, operators)

    def mix(group, gathered, weights):
        return call(
            functools.partial(mix_blocks, plane_size, plans[group]),
            [VMEM] * plane_size + [SMEM],
            blocks_of[group],
        )(*gathered, weights)

    def store(group, blocks, so_far):
        before = [] if so_far is None else [so_far]
        return call(
            functools.partial(store_rows, plane_size, rows, groups[group][0]),
            [VMEM] * plane_size + [HBM] * len(before),
            whole,
            out_specs=HBM,
            aliases={plane_size: 0} if before else None,
            scratch=[pltpu.SemaphoreType.DMA((plane_size,))],
        )(*blocks, *before)

    weights = call(
        functools.partial(make_weights, count_y, count_z),
        [SMEM, SMEM],
        jax.ShapeDtypeStruct((5, plane_size, plane_size), jnp.float32),
        out_specs=SMEM,
        scratch=[pltpu.SMEM((plane_size, plane_size), jnp.float32)],
    )(
        plane_coupling.reshape(plane_size, plane_size).astype(jnp.float32),
        face_owner.reshape(plane_size),
    )
    incoming = None
    for sweep in range(SWEEPS):
        out_yz = [None] * plane_size
        for ks in row_groups(count_y, count_z):
            for k, block in zip(ks, solve("yz", sweep, ks, incoming)):
                out_yz[k] = block
            if len(placed) == 1:
                load()
        gathered_yz = exchange(out_yz, count_y, count_z)
        low, high = solve("x", sweep, tuple(range(plane_size)), incoming)
        from_low = lax.ppermute(high, "gx", forward)
        from_high = lax.ppermute(low, "gx", backward)
        packed = call(pack_faces, [VMEM] * 2, blocks_of["x"])(from_low, from_high)
        gathered_x = exchange(packed, count_y, count_z)
        mixed_yz = mix("yz", gathered_yz, weights)
        incoming = {"yz": exchange(mixed_yz, count_y, count_z)}
        mixed_x = mix("x", gathered_x, weights)
        incoming["x"] = exchange(mixed_x, count_y, count_z)
    result = store("x", incoming["x"], store("yz", incoming["yz"], None))
    return result.reshape(traces.shape)


def solution(mesh):
    placed = (
        P(None, "gx", "gy", "gz", None, None),
        P(None, "gx", "gy", "gz", None, None),
        P(None, "gx", "gy", "gz", None, None),
        P("gx", None, None),
        P("gx", None),
    )
    counts = [mesh.shape[a] for a in ("gy", "gz")]
    few = counts[0] * counts[1] <= 8 and all(c & (c - 1) == 0 for c in counts)
    return jax.shard_map(
        few_subdomains if few else many_subdomains,
        mesh=mesh,
        in_specs=placed,
        out_specs=P(None, "gx", "gy", "gz", None, None),
        check_vma=False,
    )
```

```python
import functools

import jax
import jax.numpy as jnp
from jax import lax
from jax.experimental import pallas as pl
from jax.experimental.pallas import tpu as pltpu
from jax.sharding import PartitionSpec as P

SWEEPS = 2


def with_halo(block, sides, width):
    for axis, dim in sides:
        count = lax.axis_size(axis)
        forward = [(i, i + 1) for i in range(count - 1)]
        forward.append((count - 1, 0))
        backward = [(target, source) for source, target in forward]
        low = lax.ppermute(
            lax.slice_in_dim(block, block.shape[dim] - width, None, axis=dim), axis, forward
        )
        high = lax.ppermute(lax.slice_in_dim(block, 0, width, axis=dim), axis, backward)
        block = jnp.concatenate([low, block, high], axis=dim)
    return block


def many_subdomains(traces, sources, local_ops, plane_coupling, face_owner):
    columns_all = local_ops.shape[-1]
    slab_width = columns_all // 6
    slab_rows = traces.shape[4]
    count_y = lax.axis_size("gy")
    count_z = lax.axis_size("gz")
    plane_size = count_y * count_z
    block_rows_count = slab_rows // plane_size
    operators = local_ops.reshape(2, columns_all, columns_all)
    source_rows = sources.reshape(2, slab_rows, columns_all).astype(jnp.float32)
    incoming = traces.reshape(2, slab_rows, columns_all)
    owners = face_owner.reshape(plane_size)
    select = (owners[:, None] == jnp.arange(plane_size, dtype=jnp.int32)[None, :]).astype(
        jnp.float32
    )
    mixing = jnp.dot(
        plane_coupling.reshape(plane_size, plane_size).astype(jnp.float32),
        select,
        precision=lax.Precision.HIGHEST,
    ).astype(jnp.bfloat16)
    for _ in range(SWEEPS):
        real_part = (
            jnp.dot(incoming[0], operators[0], preferred_element_type=jnp.float32)
            - jnp.dot(incoming[1], operators[1], preferred_element_type=jnp.float32)
            + source_rows[0]
        )
        imag_part = (
            jnp.dot(incoming[0], operators[1], preferred_element_type=jnp.float32)
            + jnp.dot(incoming[1], operators[0], preferred_element_type=jnp.float32)
            + source_rows[1]
        )
        outgoing = (
            jnp.stack([real_part, imag_part])
            .astype(jnp.bfloat16)
            .reshape(2, slab_rows, 6, slab_width)
        )
        along_x = with_halo(outgoing[:, :, 0:2, :], (("gx", 2),), 1)
        partial_faces = jnp.concatenate(
            [along_x[:, :, 0:1], along_x[:, :, 3:4], outgoing[:, :, 2:6]], axis=2
        )
        blocks = partial_faces.reshape(2, plane_size, block_rows_count, 6, slab_width)
        update_block_rows = lax.all_to_all(
            blocks, ("gy", "gz"), split_axis=1, concat_axis=1, tiled=True
        )
        row_count = update_block_rows.shape[2]
        grid_view = update_block_rows.reshape(2, count_y, count_z, row_count, 6, slab_width)
        moved = jnp.stack(
            [
                grid_view[:, :, :, :, 0],
                grid_view[:, :, :, :, 1],
                jnp.roll(grid_view[:, :, :, :, 3], 1, axis=1),
                jnp.roll(grid_view[:, :, :, :, 2], -1, axis=1),
                jnp.roll(grid_view[:, :, :, :, 5], 1, axis=2),
                jnp.roll(grid_view[:, :, :, :, 4], -1, axis=2),
            ],
            axis=4,
        )
        block_rows = moved.reshape(2, plane_size, row_count * columns_all)
        coupled = jnp.einsum("pq,rqc->rpc", mixing, block_rows, preferred_element_type=jnp.float32)
        updated = (block_rows.astype(jnp.float32) - coupled).astype(jnp.bfloat16)
        updated = updated.reshape(2, plane_size, row_count, 6, slab_width)
        returned = lax.all_to_all(updated, ("gy", "gz"), split_axis=1, concat_axis=1, tiled=True)
        incoming = returned.reshape(2, slab_rows, columns_all)
    return incoming.reshape(traces.shape)


VMEM = pl.BlockSpec(memory_space=pltpu.VMEM)
SMEM = pl.BlockSpec(memory_space=pltpu.SMEM)
HBM = pl.BlockSpec(memory_space=pltpu.HBM)
KERNEL_BYTES = 24 << 20
FIRST_BYTES = 53 << 20
LOAD_BYTES = 50 << 20
KERNEL_FLOPS = 1 << 31


def plane_position():
    return lax.axis_index("gy") * lax.axis_size("gz") + lax.axis_index("gz")


def call(kernel, in_specs, out_shape, out_specs=None, aliases=None, scratch=(), limit=KERNEL_BYTES):
    return pl.pallas_call(
        kernel,
        in_specs=in_specs,
        out_shape=out_shape,
        out_specs=out_specs if out_specs is not None else jax.tree.map(lambda _: VMEM, out_shape),
        scratch_shapes=scratch,
        input_output_aliases=aliases or {},
        cost_estimate=pl.CostEstimate(
            flops=KERNEL_FLOPS, bytes_accessed=1 << 20, transcendentals=0
        ),
        compiler_params=pltpu.CompilerParams(vmem_limit_bytes=limit),
    )


def row_start(k, rows):
    return pl.multiple_of((plane_position() ^ k) * rows, rows)


def part_products(part, real, imag, operators):
    if part == 0:
        return jnp.dot(real, operators[0], preferred_element_type=jnp.float32) - jnp.dot(
            imag, operators[1], preferred_element_type=jnp.float32
        )
    return jnp.dot(real, operators[1], preferred_element_type=jnp.float32) + jnp.dot(
        imag, operators[0], preferred_element_type=jnp.float32
    )


def start_all(pairs, sems):
    copies = [
        pltpu.make_async_copy(source, target, sems.at[n]) for n, (source, target) in enumerate(pairs)
    ]
    for copy in copies:
        copy.start()
    return copies


def load_and_solve(ks, rows, first, columns, traces_ref, sources_ref, operators_ref, *refs):
    blocks, operators, (traces, sources, sems) = refs[: len(ks)], refs[len(ks)], refs[-3:]
    wanted = pl.ds(first, columns)
    here = [pl.ds(row_start(k, rows), rows) for k in ks]
    pairs = [(operators_ref.at[part, :, wanted], operators.at[part]) for part in range(2)]
    pairs += [(traces_ref.at[:, r, :], traces.at[n]) for n, r in enumerate(here)]
    pairs += [(sources_ref.at[:, r, wanted], sources.at[n]) for n, r in enumerate(here)]
    copies = start_all(pairs, sems)
    needed, late = copies[: -len(ks)], copies[-len(ks) :]
    for copy in needed:
        copy.wait()
    real, imag = (
        jnp.concatenate([traces[n, part] for n in range(len(ks))], axis=0) for part in range(2)
    )
    results = [part_products(part, real, imag, operators) for part in range(2)]
    for copy in late:
        copy.wait()
    finish(range(len(ks)), rows, slice(0, columns), pick_block, results, sources, blocks)


def load_rest(
    plane_size, rows, first, columns, traces_ref, sources_ref, operators_ref, traces, sources, operators, sems
):
    pairs = []
    for source, target in ((traces_ref, traces), (sources_ref, sources)):
        for k in range(plane_size):
            pairs.append((source.at[:, pl.ds(row_start(k, rows), rows), :], target.at[k]))
    pairs.append((operators_ref.at[:, :, pl.ds(first, columns)], operators))
    for copy in start_all(pairs, sems):
        copy.wait()


def finish(ks, rows, wanted, pick, results, sources, outputs):
    for part, result in enumerate(results):
        for n, k in enumerate(ks):
            block = result[n * rows : (n + 1) * rows] + sources[k, part, :, wanted].astype(
                jnp.float32
            )
            pick(outputs, part, n, block.astype(outputs[0].dtype))


def solve_blocks(ks, rows, first, columns, pick, count, *refs):
    wanted = slice(first, first + columns)
    if count == 1:
        traces, sources, operators_ref = refs[:3]
        outputs = refs[3:]
        pieces = [[jnp.concatenate([traces[k, part] for k in ks], axis=0) for part in range(2)]]
    else:
        incoming, (sources, operators_ref) = refs[: 2 * len(ks)], refs[2 * len(ks) : 2 * len(ks) + 2]
        outputs = refs[2 * len(ks) + 2 :]
        pieces = [
            [jnp.concatenate([b[part] for b in group], axis=0) for part in range(2)]
            for group in (incoming[: len(ks)], incoming[len(ks) :])
        ]
    results = [0.0, 0.0]
    start = 0
    for real, imag in pieces:
        depth = slice(start, start + real.shape[-1])
        start = depth.stop
        operators = [operators_ref[part, depth] for part in range(2)]
        for part in range(2):
            results[part] = results[part] + part_products(part, real, imag, operators)
    finish(ks, rows, wanted, pick, results, sources, outputs)


def pick_block(outputs, part, k, block):
    outputs[k][part] = block


def pick_face(outputs, part, k, block):
    width = block.shape[-1] // 2
    outputs[0][k, part] = block[:, :width]
    outputs[1][k, part] = block[:, width:]


def pack_faces(from_low_ref, from_high_ref, *outputs):
    width = from_low_ref.shape[-1]
    for k, output in enumerate(outputs):
        output[:, :, :width] = from_low_ref[k]
        output[:, :, width:] = from_high_ref[k]


def make_weights(count_y, count_z, coupling_ref, owner_ref, weights_ref, column_ref):
    plane_size = count_y * count_z
    me = plane_position()

    def clear(q, carry):
        for p in range(plane_size):
            column_ref[p, q] = jnp.where(p == q, jnp.float32(1), jnp.float32(0))
        return carry

    def couple(q, carry):
        owner = owner_ref[q]
        for p in range(plane_size):
            column_ref[p, owner] = column_ref[p, owner] - coupling_ref[p, q]
        return carry

    lax.fori_loop(0, plane_size, clear, 0)
    lax.fori_loop(0, plane_size, couple, 0)

    def fill(m, carry):
        source = me ^ m
        y, z = source // count_z, source % count_z
        receivers = (
            source,
            ((y + 1) % count_y) * count_z + z,
            ((y + count_y - 1) % count_y) * count_z + z,
            y * count_z + (z + 1) % count_z,
            y * count_z + (z + count_z - 1) % count_z,
        )
        for face, receiver in enumerate(receivers):
            for k in range(plane_size):
                weights_ref[face, k, m] = column_ref[me ^ k, receiver]
        return carry

    lax.fori_loop(0, plane_size, fill, 0)


def mix_blocks(plane_size, plan, *refs):
    blocks, weights_ref, outputs = refs[:plane_size], refs[plane_size], refs[plane_size + 1 :]
    width = blocks[0].shape[-1] // len(plan)
    for face, (kind, source_face) in enumerate(plan):
        columns = slice(source_face * width, (source_face + 1) * width)
        for part in range(2):
            values = [b[part, :, columns].astype(jnp.float32) for b in blocks]
            for k, output in enumerate(outputs):
                total = values[0] * weights_ref[kind, k, 0]
                for m in range(1, plane_size):
                    total = total + values[m] * weights_ref[kind, k, m]
                output[part, :, face * width : (face + 1) * width] = total.astype(output.dtype)


def store_rows(plane_size, rows, first, *refs):
    blocks, out_ref, sems = refs[:plane_size], refs[-2], refs[-1]
    columns = blocks[0].shape[-1]
    copies = [
        pltpu.make_async_copy(
            blocks[k],
            out_ref.at[:, pl.ds(row_start(k, rows), rows), pl.ds(first, columns)],
            sems.at[k],
        )
        for k in range(plane_size)
    ]
    for copy in copies:
        copy.start()
    for copy in copies:
        copy.wait()


def partners(count_y, count_z):
    across = range(1, count_y * count_z)
    far = [k for k in across if 2 * (k // count_z) >= count_y]
    near = [k for k in across if k not in far]
    return sorted(far, key=lambda k: (k % count_z, k)) + sorted(
        near, key=lambda k: (-(k % count_z), k)
    )


def far_and_near(count_y, count_z):
    ks = partners(count_y, count_z)
    far = tuple(k for k in ks if 2 * (k // count_z) >= count_y)
    return far, tuple(k for k in ks if k not in far)


def row_groups(count_y, count_z):
    far, near = far_and_near(count_y, count_z)
    half = len(far) // 2
    return [ks for ks in (far[:half], far[half:], (0,) + near) if ks]


def exchange(blocks, count_y, count_z):
    plane_size = count_y * count_z
    received = [blocks[0]] + [None] * (plane_size - 1)
    for k in partners(count_y, count_z):
        received[k] = lax.ppermute(blocks[k], ("gy", "gz"), [(p, p ^ k) for p in range(plane_size)])
    return received


def few_subdomains(traces, sources, local_ops, plane_coupling, face_owner):
    columns_all = local_ops.shape[-1]
    width = columns_all // 6
    slab_rows = traces.shape[4]
    count_x, count_y, count_z = (lax.axis_size(a) for a in ("gx", "gy", "gz"))
    plane_size = count_y * count_z
    rows = slab_rows // plane_size
    operators = local_ops.reshape(2, columns_all, columns_all)
    source_rows = sources.reshape(2, slab_rows, columns_all)
    trace_rows = traces.reshape(2, slab_rows, columns_all)
    dtype = traces.dtype
    forward = [(i, (i + 1) % count_x) for i in range(count_x)]
    backward = [(target, source) for source, target in forward]
    whole = jax.ShapeDtypeStruct((2, slab_rows, columns_all), dtype)
    groups = {"x": (0, 2 * width), "yz": (2 * width, 4 * width)}
    plans = {"x": ((0, 0), (0, 1)), "yz": ((1, 1), (2, 0), (3, 3), (4, 2))}
    face = jax.ShapeDtypeStruct((plane_size, 2, rows, width), dtype)
    blocks_of = {
        g: [jax.ShapeDtypeStruct((2, rows, columns), dtype)] * plane_size
        for g, (_, columns) in groups.items()
    }
    solved = {"x": ([face] * 2, pick_face), "yz": (blocks_of["yz"], pick_block)}

    placed = {}

    def solve(group, sweep, ks, incoming):
        first, columns = groups[group]
        out_shape, pick = solved[group]
        if group == "yz":
            out_shape = out_shape[: len(ks)]
        if not placed:
            *blocks, placed[group] = call(
                functools.partial(load_and_solve, ks, rows, first, columns),
                [HBM] * 3,
                out_shape + [jax.ShapeDtypeStruct((2, columns_all, columns), dtype)],
                scratch=[
                    pltpu.VMEM((len(ks), 2, rows, columns_all), dtype),
                    pltpu.VMEM((len(ks), 2, rows, columns), dtype),
                    pltpu.SemaphoreType.DMA((2 * len(ks) + 2,)),
                ],
                limit=FIRST_BYTES,
            )(trace_rows, source_rows, operators)
            return blocks
        if sweep == 0:
            arrays = [placed["traces"]]
        else:
            arrays = [incoming[g][k] for g in ("x", "yz") for k in ks]
        return call(
            functools.partial(solve_blocks, ks, rows, first, columns, pick, 1 if sweep == 0 else 2),
            [VMEM] * (len(arrays) + 2),
            out_shape,
        )(*arrays, placed["sources"], placed[group])

    def load():
        first, columns = groups["x"]
        by_block = jax.ShapeDtypeStruct((plane_size, 2, rows, columns_all), dtype)
        placed["traces"], placed["sources"], placed["x"] = call(
            functools.partial(load_rest, plane_size, rows, first, columns),
            [HBM] * 3,
            [by_block, by_block, jax.ShapeDtypeStruct((2, columns_all, columns), dtype)],
            scratch=[pltpu.SemaphoreType.DMA((2 * plane_size + 1,))],
            limit=LOAD_BYTES,
        )(trace_rows, source_rows, operators)

    def mix(group, gathered, weights):
        return call(
            functools.partial(mix_blocks, plane_size, plans[group]),
            [VMEM] * plane_size + [SMEM],
            blocks_of[group],
        )(*gathered, weights)

    def store(group, blocks, so_far):
        before = [] if so_far is None else [so_far]
        return call(
            functools.partial(store_rows, plane_size, rows, groups[group][0]),
            [VMEM] * plane_size + [HBM] * len(before),
            whole,
            out_specs=HBM,
            aliases={plane_size: 0} if before else None,
            scratch=[pltpu.SemaphoreType.DMA((plane_size,))],
        )(*blocks, *before)

    weights = call(
        functools.partial(make_weights, count_y, count_z),
        [SMEM, SMEM],
        jax.ShapeDtypeStruct((5, plane_size, plane_size), jnp.float32),
        out_specs=SMEM,
        scratch=[pltpu.SMEM((plane_size, plane_size), jnp.float32)],
    )(
        plane_coupling.reshape(plane_size, plane_size).astype(jnp.float32),
        face_owner.reshape(plane_size),
    )
    incoming = None
    for sweep in range(SWEEPS):
        out_yz = [None] * plane_size
        for ks in row_groups(count_y, count_z):
            for k, block in zip(ks, solve("yz", sweep, ks, incoming)):
                out_yz[k] = block
            if len(placed) == 1:
                load()
        gathered_yz = exchange(out_yz, count_y, count_z)
        low, high = solve("x", sweep, tuple(range(plane_size)), incoming)
        from_low = lax.ppermute(high, "gx", forward)
        from_high = lax.ppermute(low, "gx", backward)
        packed = call(pack_faces, [VMEM] * 2, blocks_of["x"])(from_low, from_high)
        gathered_x = exchange(packed, count_y, count_z)
        mixed_yz = mix("yz", gathered_yz, weights)
        incoming = {"yz": exchange(mixed_yz, count_y, count_z)}
        mixed_x = mix("x", gathered_x, weights)
        incoming["x"] = exchange(mixed_x, count_y, count_z)
    result = store("x", incoming["x"], store("yz", incoming["yz"], None))
    return result.reshape(traces.shape)


def solution(mesh):
    placed = (
        P(None, "gx", "gy", "gz", None, None),
        P(None, "gx", "gy", "gz", None, None),
        P(None, "gx", "gy", "gz", None, None),
        P("gx", None, None),
        P("gx", None),
    )
    counts = [mesh.shape[a] for a in ("gy", "gz")]
    few = counts[0] * counts[1] <= 8 and all(c & (c - 1) == 0 for c in counts)
    return jax.shard_map(
        few_subdomains if few else many_subdomains,
        mesh=mesh,
        in_specs=placed,
        out_specs=P(None, "gx", "gy", "gz", None, None),
        check_vma=False,
    )
```
